1024 devices in a mesh: dp: 16 (over y, core), tensor: 8 (over x), pipe: 8 (over z).
Axes of the slice: x: 8, y: 8, z: 8, core: 2. Of those that a mesh axis runs over, the one named last changes fastest.
Arguments:
- grad_parts: float32 [16, 8, 8, 64, 8192], P('dp', 'pipe', 'tensor'), may hold values from -24 to 24
- drop_flags: int32 [16, 8, 8, 64], P('dp', 'pipe', 'tensor'), may hold values from 0 to 1, as said below
- owner_order: int32 [16], replicated, may hold values from 0 to 15, each once
- step_count: int32 [], replicated, may hold values from 1 to 11
- master: float32 [8, 8, 64, 8192], P('pipe', 'tensor', None, 'dp'), may hold values from -6 to 6
- moment_m: float32 [8, 8, 64, 8192], P('pipe', 'tensor', None, 'dp'), may hold values from -0.15625 to 0.15625
- moment_v: float32 [8, 8, 64, 8192], P('pipe', 'tensor', None, 'dp'), may hold values from 0.0001 to 0.001
Outputs:
- new_master: float32 [8, 8, 64, 8192], P('pipe', 'tensor', None, 'dp')
- new_m: float32 [8, 8, 64, 8192], P('pipe', 'tensor', None, 'dp')
- new_v: float32 [8, 8, 64, 8192], P('pipe', 'tensor', None, 'dp')
- direction: float32 [8, 8, 64, 8192], P('pipe', 'tensor', None, 'dp')
- dropped_total: int32 [], replicated
The draws below stay inside these ranges and needn't reach their ends.
Inputs may be any that keep to these rules, and one draw needn't show every extreme that they name: `drop_flags`: A row may be flagged by every replica.
All inputs are finite; a program needn't handle non-finite values.
Results may differ from the reference program's by a relative error of at most 0.0003.
Values sent between devices are 32-bit elements; how exact they have to be, the bound alone decides.
A program may use at most 32 MiB of HBM per device.

```python
import math
import jax
import jax.numpy as jnp
from jax import lax

D = 8192
ROWS = 64
LAYERS = 8
SHARDS = 8
N_DP = 16


def draw_drop_flags(key, part):
    random_ones = jax.random.randint(jax.random.fold_in(key, 11), (N_DP, LAYERS, SHARDS, ROWS), 0, 4) == 0
    full_rows = jax.random.randint(jax.random.fold_in(key, 12), (LAYERS, SHARDS, ROWS), 0, 32) == 0
    forced = jax.random.randint(jax.random.fold_in(key, 13), (), 0, LAYERS * SHARDS * ROWS)
    position = jnp.arange(LAYERS * SHARDS * ROWS, dtype=jnp.int32).reshape(LAYERS, SHARDS, ROWS)
    every_replica = full_rows | (position == forced)
    return jnp.where(random_ones | every_replica[None], 1, 0).astype(jnp.int32)


def draw_grad_parts(key, part):
    block_cols = D // N_DP
    pairing = jax.random.permutation(jax.random.fold_in(key, 21), N_DP)
    column_block = jnp.arange(D, dtype=jnp.int32) // block_cols
    spiked = column_block[None, :] == pairing[:, None]
    factor = jnp.where(spiked, 4.0, 1.0).astype(jnp.float32)[:, None, None, None, :]
    noise = jax.random.normal(jax.random.fold_in(key, 22), (N_DP, LAYERS, SHARDS, ROWS, D), jnp.float32)
    own_part = jnp.clip(noise, -6.0, 6.0) * factor
    values = own_part
    return values.astype(jnp.float32)


def levels(own_key, dims, pieces, low, top_value):
    gain = 1.0
    for axis_at, shards_of in pieces:
        heights = jax.random.uniform(jax.random.fold_in(jax.random.fold_in(own_key, 6), axis_at), (shards_of,), jnp.float32, low / len(pieces), top_value / len(pieces))
        gain = gain * jnp.repeat(jnp.exp(heights), dims[axis_at] // shards_of).reshape((-1,) + (1,) * (len(dims) - 1 - axis_at))
    return gain


def gaussian(key, shape, spread, most, pieces=(), kind=jnp.bfloat16):
    array = jax.random.normal(key, shape, jnp.float32) * spread
    if len(pieces) > 0:
        array = levels(key, shape, pieces, -0.22, 0.18) * array
    return jnp.clip(array, min=-most, max=most).astype(kind)


def setup_inputs(seed: int = 0) -> dict:
    streams_of = jax.random.split(jax.random.key(seed), 8)
    return {
        "grad_parts": draw_grad_parts(jax.random.fold_in(streams_of[7], 71), 0),
        "drop_flags": draw_drop_flags(jax.random.fold_in(streams_of[7], 71), 0),
        "owner_order": jax.random.permutation(streams_of[2], N_DP).astype(jnp.int32),
        "step_count": jax.random.randint(streams_of[3], (), 1, 12).astype(jnp.int32),
        "master": gaussian(streams_of[4], (LAYERS, SHARDS, ROWS, D), 1.0, 6.0, ((0, 8), (1, 8), (3, 16)), jnp.float32),
        "moment_m": gaussian(streams_of[5], (LAYERS, SHARDS, ROWS, D), 0.01, 0.15625, ((0, 8), (1, 8), (3, 16)), jnp.float32),
        "moment_v": jnp.clip(jnp.exp(math.log(0.001) - 2.3025852 * jax.random.uniform(streams_of[6], (LAYERS, SHARDS, ROWS, D), jnp.float32) ** levels(streams_of[6], (LAYERS, SHARDS, ROWS, D), ((0, 8), (1, 8), (3, 16)), -0.2, 0.2)), 0.0001, 0.001),
    }


def reference(grad_parts, drop_flags, owner_order, step_count, master, moment_m, moment_v):
    kept = (1 - drop_flags).astype(jnp.float32)

    def accumulate(carry, pair):
        part, keep = pair
        return ((carry[0] + part * keep[..., None], carry[1] + keep), None)
    start = (jnp.zeros(grad_parts.shape[1:], jnp.float32), jnp.zeros(kept.shape[1:], jnp.float32))
    (total, count), unused = lax.scan(accumulate, start, (grad_parts, kept))
    mean_grad = total / jnp.maximum(count, 1.0)[..., None]
    shape = mean_grad.shape
    blocks = mean_grad.reshape(shape[0], shape[1], shape[2], N_DP, shape[3] // N_DP)
    grad = jnp.take(blocks, owner_order, axis=3).reshape(shape)
    entries = shape[0] * shape[1] * shape[2] * shape[3]
    rms = jnp.sqrt(jnp.sum(grad * grad) / entries)
    clip = jnp.minimum(1.0, 0.05 / (rms + 1e-06))
    scaled = clip * grad
    new_m = 0.9 * moment_m + 0.1 * scaled
    new_v = 0.999 * moment_v + 0.001 * scaled * scaled
    steps = step_count.astype(jnp.float32)
    m_hat = new_m / (1.0 - jnp.power(0.9, steps))
    v_hat = new_v / (1.0 - jnp.power(0.999, steps))
    direction = m_hat / (jnp.sqrt(v_hat) + 1e-08) + 0.1 * master
    new_master = master - 0.001 * direction
    dropped_total = jnp.sum(drop_flags).astype(jnp.int32)
    return (new_master, new_m, new_v, direction, dropped_total)
```

```python
import jax
import jax.numpy as jnp
from jax import lax
from jax.experimental import pallas as pl
from jax.experimental.pallas import tpu as pltpu
from jax.sharding import Mesh
from jax.sharding import PartitionSpec as P

MESH = pl.DeviceIdType.MESH
Y = 8
ROWS, COLS = 64, 512
WIDTH = 2 * Y * COLS
HALF = ROWS // 2
ENTRIES = 33554432.0

D_ORDER = (4, 3, 5, 2, 6, 1, 7, 0)
UP = ((4, 0), (3, 1), (3, 0), (2, 1), (2, 0), (1, 1), (1, 0))
DOWN = ((4, 1), (3, 0), (3, 1), (2, 0), (2, 1), (1, 0), (1, 1))


def kernel(
    order, steps, flags, grad, master, moment_m, moment_v,
    out_w, out_m, out_v, out_d, out_drop,
    order_s, steps_s, flags_v, x, st, dsend, drecv, ring_send, ring_recv, fsend, frecv, csend, crecv, nsend, nrecv,
    load_sem, small_sem, st_sem, d_ss, d_rs, r_ss, r_rs, f_ss, f_rs, c_ss, c_rs, n_ss, n_rs,
):
    y = lax.axis_index("y")
    c = lax.axis_index("c")
    tx = lax.axis_index("tensor")
    pz = lax.axis_index("pipe")
    other = 1 - c

    barrier = pltpu.get_barrier_semaphore()
    pl.semaphore_signal(barrier, inc=1, device_id={"c": other}, device_id_type=MESH)
    for o in range(1, 8):
        pl.semaphore_signal(barrier, inc=1, device_id={"y": lax.rem(y + o, 8)}, device_id_type=MESH)
        pl.semaphore_signal(barrier, inc=1, device_id={"tensor": lax.rem(tx + o, 8)}, device_id_type=MESH)
        pl.semaphore_signal(barrier, inc=1, device_id={"pipe": lax.rem(pz + o, 8)}, device_id_type=MESH)

    smalls = [
        pltpu.make_async_copy(ref, to, small_sem.at[i])
        for i, (ref, to) in enumerate(((flags, flags_v), (order, order_s), (steps, steps_s)))
    ]
    for s in smalls:
        s.start()
    loads = [
        pltpu.make_async_copy(grad.at[:, pl.ds(b * COLS, COLS)], x.at[b], load_sem.at[b])
        for b in range(2 * Y)
    ]
    for s in loads:
        s.start()
    states = [
        pltpu.make_async_copy(ref, st.at[i], st_sem.at[i])
        for i, ref in enumerate((master, moment_m, moment_v))
    ]
    for s in states:
        s.start()

    for s in smalls:
        s.wait()
    flag_row = flags_v[...].astype(jnp.float32)
    kept_row = 1.0 - flag_row
    eye = lax.broadcasted_iota(jnp.int32, (ROWS, ROWS), 0) == lax.broadcasted_iota(
        jnp.int32, (ROWS, ROWS), 1
    )

    def as_column(row):
        return jnp.sum(jnp.where(eye, jnp.broadcast_to(row, (ROWS, ROWS)), 0.0), axis=1, keepdims=True)

    kept = as_column(kept_row)
    fsend[...] = jnp.concatenate([kept_row, jnp.zeros((1, 128 - ROWS), jnp.float32)], axis=1)

    def mine(chip, core, lo, n):
        return x[order_s[2 * chip + core], lo : lo + n] * kept[lo : lo + n]

    for s in loads:
        s.wait()
    pl.semaphore_wait(barrier, 22)

    d_copies = {}
    for d in D_ORDER:
        chip = lax.rem(y + d, 8)
        dsend[d] = mine(chip, other, 0, ROWS)
        cp = pltpu.make_async_remote_copy(
            src_ref=dsend.at[d], dst_ref=drecv.at[d], send_sem=d_ss.at[d], recv_sem=d_rs.at[d],
            device_id={"c": other}, device_id_type=MESH,
        )
        cp.start()
        d_copies[d] = cp
    f_copy = pltpu.make_async_remote_copy(
        src_ref=fsend, dst_ref=frecv, send_sem=f_ss, recv_sem=f_rs,
        device_id={"c": other}, device_id_type=MESH,
    )
    f_copy.start()

    def on_chip(d, half):
        chip = lax.rem(y + d, 8)
        lo = half * HALF
        return mine(chip, c, lo, HALF) + drecv[d, lo : lo + HALF]

    seen = set()
    sends = []
    waited = set()

    def ring_copy(way, k, half):
        lo = half * HALF
        i = (way * 4 + (k - 1)) * 2 + half
        to = lax.rem(y + (1 if way == 0 else 7), 8)
        return pltpu.make_async_remote_copy(
            src_ref=ring_send.at[way, k - 1, pl.ds(lo, HALF)],
            dst_ref=ring_recv.at[way, k - 1, pl.ds(lo, HALF)],
            send_sem=r_ss.at[i], recv_sem=r_rs.at[i],
            device_id={"y": to}, device_id_type=MESH,
        )

    def stage(way, k, half):
        d = k if way == 0 else 8 - k
        if d not in seen:
            d_copies[d].wait_recv()
            seen.add(d)
        lo = half * HALF
        value = on_chip(d, half)
        top = 4 if half == way else 3
        if k < top:
            ring_copy(way, k + 1, half).wait_recv()
            value = value + ring_recv[way, k, lo : lo + HALF]
        ring_send[way, k - 1, lo : lo + HALF] = value
        cp = ring_copy(way, k, half)
        cp.start()
        sends.append(cp)

    c_copies = []
    for i in range(7):
        stage(0, *UP[i])
        stage(1, *DOWN[i])
        if i == 1:
            f_copy.wait_recv()
            csend[...] = fsend[...] + frecv[...]
            for o in range(1, 8):
                cp = pltpu.make_async_remote_copy(
                    src_ref=csend, dst_ref=crecv.at[o], send_sem=c_ss.at[o], recv_sem=c_rs.at[o],
                    device_id={"y": lax.rem(y + o, 8)}, device_id_type=MESH,
                )
                cp.start()
                c_copies.append(cp)

    for cp in c_copies:
        cp.wait_recv()
    count_row = csend[...]
    for o in range(1, 8):
        count_row = count_row + crecv[o]
    count = jnp.maximum(as_column(count_row[:, :ROWS]), 1.0)

    d_copies[0].wait_recv()
    squares = jnp.zeros((8, COLS), jnp.float32)
    means = []
    for half in (1, 0):
        lo = half * HALF
        part = on_chip(0, half)
        for way in ((0, 1) if half else (1, 0)):
            ring_copy(way, 1, half).wait_recv()
            part = part + ring_recv[way, 0, lo : lo + HALF]
        mean = part / count[lo : lo + HALF]
        means.append(mean)
        sq = mean * mean
        for r in range(0, HALF, 8):
            squares = squares + sq[r : r + 8]
    mean = jnp.concatenate([means[1], means[0]], axis=0)
    squares = squares[:, 0:128] + squares[:, 128:256] + squares[:, 256:384] + squares[:, 384:512]
    squares = jnp.sum(squares, axis=0, keepdims=True)

    message = jnp.concatenate(
        [squares, jnp.concatenate([flag_row, jnp.zeros((1, 128 - ROWS), jnp.float32)], axis=1)], axis=0
    )

    def exchange(phase, peers, message):
        nsend[phase] = message
        copies = []
        for o, peer in peers:
            cp = pltpu.make_async_remote_copy(
                src_ref=nsend.at[phase], dst_ref=nrecv.at[phase * 8 + o],
                send_sem=n_ss.at[phase * 8 + o], recv_sem=n_rs.at[phase * 8 + o],
                device_id=peer, device_id_type=MESH,
            )
            cp.start()
            copies.append(cp)
        for (o, _), cp in zip(peers, copies):
            cp.wait_recv()
            message = message + nrecv[phase * 8 + o]
        sends.extend(copies)
        return message

    message = exchange(0, [(0, {"c": other})], message)
    message = exchange(1, [(o, {"tensor": lax.rem(tx + o, 8)}) for o in range(1, 8)], message)
    message = exchange(2, [(o, {"pipe": lax.rem(pz + o, 8)}) for o in range(1, 8)], message)
    message = exchange(3, [(o, {"y": lax.rem(y + o, 8)}) for o in range(1, 8)], message)
    totals = jnp.sum(message, axis=1, keepdims=True)
    rms = jnp.sqrt(totals[0:1] / ENTRIES)
    clip = jnp.minimum(1.0, 0.05 / (rms + 1e-6))
    out_drop[0] = totals[1, 0].astype(jnp.int32)

    t = jnp.full((8, 128), steps_s[0], jnp.int32)

    def power(base):
        result = jnp.ones((8, 128), jnp.float32)
        factor = jnp.full((8, 128), base, jnp.float32)
        for bit in range(5):
            result = jnp.where(((t >> bit) & 1) == 1, result * factor, result)
            factor = factor * factor
        return result

    bias1 = (1.0 - power(0.9))[0:1, 0:1]
    bias2 = (1.0 - power(0.999))[0:1, 0:1]

    for s in states:
        s.wait()
    g = mean * clip
    w = st[0]
    new_m = 0.9 * st[1] + 0.1 * g
    new_v = 0.999 * st[2] + 0.001 * g * g
    direction = (new_m / bias1) / (jnp.sqrt(new_v / bias2) + 1e-8) + 0.1 * w
    out_m[...] = new_m
    out_v[...] = new_v
    out_d[...] = direction
    out_w[...] = w - 0.001 * direction

    f_copy.wait_send()
    for cp in (*d_copies.values(), *c_copies, *sends):
        cp.wait_send()


def body(grad_parts, drop_flags, owner_order, step_count, master, moment_m, moment_v):
    block = jax.ShapeDtypeStruct((ROWS, COLS), jnp.float32)
    dma = pltpu.SemaphoreType.DMA
    vmem = pl.BlockSpec(memory_space=pltpu.VMEM)
    smem = pl.BlockSpec(memory_space=pltpu.SMEM)
    hbm = pl.BlockSpec(memory_space=pltpu.HBM)
    f32 = jnp.float32
    new_w, new_m, new_v, direction, dropped = pl.pallas_call(
        kernel,
        out_shape=(block, block, block, block, jax.ShapeDtypeStruct((1,), jnp.int32)),
        in_specs=[hbm] * 7,
        out_specs=(vmem, vmem, vmem, vmem, smem),
        scratch_shapes=[
            pltpu.SMEM((2 * Y,), jnp.int32),
            pltpu.SMEM((1,), jnp.int32),
            pltpu.VMEM((1, ROWS), jnp.int32),
            pltpu.VMEM((2 * Y, ROWS, COLS), f32),
            pltpu.VMEM((3, ROWS, COLS), f32),
            pltpu.VMEM((8, ROWS, COLS), f32),
            pltpu.VMEM((8, ROWS, COLS), f32),
            pltpu.VMEM((2, 4, ROWS, COLS), f32),
            pltpu.VMEM((2, 4, ROWS, COLS), f32),
            pltpu.VMEM((1, 128), f32),
            pltpu.VMEM((1, 128), f32),
            pltpu.VMEM((1, 128), f32),
            pltpu.VMEM((8, 1, 128), f32),
            pltpu.VMEM((4, 2, 128), f32),
            pltpu.VMEM((32, 2, 128), f32),
            dma((16,)), dma((3,)), dma((3,)), dma((8,)), dma((8,)), dma((16,)), dma((16,)),
            dma, dma, dma((8,)), dma((8,)), dma((32,)), dma((32,)),
        ],
        compiler_params=pltpu.CompilerParams(
            collective_id=0, has_side_effects=True, vmem_limit_bytes=60 * 1024 * 1024
        ),
        name="clipped_adamw",
    )(
        owner_order,
        step_count.reshape(1),
        drop_flags.reshape(1, ROWS),
        grad_parts.reshape(ROWS, WIDTH),
        master.reshape(ROWS, COLS),
        moment_m.reshape(ROWS, COLS),
        moment_v.reshape(ROWS, COLS),
    )
    shape = (1, 1, ROWS, COLS)
    return (
        new_w.reshape(shape), new_m.reshape(shape), new_v.reshape(shape),
        direction.reshape(shape), dropped.reshape(()),
    )


def solution(mesh):
    finer = Mesh(
        mesh.devices.reshape(Y, 2, mesh.shape["tensor"], mesh.shape["pipe"]),
        ("y", "c", "tensor", "pipe"),
    )
    dp = ("y", "c")
    state = P("pipe", "tensor", None, dp)
    return jax.shard_map(
        body,
        mesh=finer,
        in_specs=(
            P(dp, "pipe", "tensor", None, None), P(dp, "pipe", "tensor", None), P(), P(),
            state, state, state,
        ),
        out_specs=(state, state, state, state, P()),
        check_vma=False,
    )
```

```python
import jax
import jax.numpy as jnp
from jax import lax
from jax.experimental import pallas as pl
from jax.experimental.pallas import tpu as pltpu
from jax.sharding import Mesh
from jax.sharding import PartitionSpec as P

MESH = pl.DeviceIdType.MESH
Y = 8
ROWS, COLS = 64, 512
WIDTH = 2 * Y * COLS
HALF = ROWS // 2
ENTRIES = 33554432.0

D_ORDER = (4, 3, 5, 2, 6, 1, 7, 0)
UP = ((4, 0), (3, 1), (3, 0), (2, 1), (2, 0), (1, 1), (1, 0))
DOWN = ((4, 1), (3, 0), (3, 1), (2, 0), (2, 1), (1, 0), (1, 1))


PLANE_ORDER = [8 * dx + dz for dz in (1, 2, 3, 4, 5, 6, 7, 0) for dx in (4, 3, 5, 2, 6, 1, 7, 0) if dx or dz]


def kernel(
    order, steps, flags, grad, out_g, out_b1, out_b2, out_drop,
    order_s, flags_v, x, dsend, drecv, ring_send, ring_recv, fsend, frecv, csend, crecv, lsend, lrecv, psend, precv,
    load_sem, small_sem, d_ss, d_rs, r_ss, r_rs, f_ss, f_rs, c_ss, c_rs, n_ss, n_rs,
):
    y = lax.axis_index("y")
    c = lax.axis_index("c")
    tx = lax.axis_index("tensor")
    pz = lax.axis_index("pipe")
    other = 1 - c

    smalls = [
        pltpu.make_async_copy(ref, to, small_sem.at[i])
        for i, (ref, to) in enumerate(((flags, flags_v), (order, order_s)))
    ]
    for s in smalls:
        s.start()
    loads = [
        pltpu.make_async_copy(grad.at[:, pl.ds(b * COLS, COLS)], x.at[b], load_sem.at[b])
        for b in range(2 * Y)
    ]
    for s in loads:
        s.start()
    line = [{"c": other}] + [
        {"y": lax.rem(y + o // 2, 8), "c": lax.rem(c + o % 2, 2)} for o in range(2, 16)
    ]
    plane = [
        {"tensor": lax.rem(tx + o // 8, 8), "pipe": lax.rem(pz + o % 8, 8)} for o in PLANE_ORDER
    ]
    barrier = pltpu.get_barrier_semaphore()
    for peer in line + plane:
        pl.semaphore_signal(barrier, inc=1, device_id=peer, device_id_type=MESH)

    for s in smalls:
        s.wait()
    flag_row = flags_v[...].astype(jnp.float32)
    kept_row = 1.0 - flag_row
    eye = lax.broadcasted_iota(jnp.int32, (ROWS, ROWS), 0) == lax.broadcasted_iota(
        jnp.int32, (ROWS, ROWS), 1
    )

    def as_column(row):
        return jnp.sum(jnp.where(eye, jnp.broadcast_to(row, (ROWS, ROWS)), 0.0), axis=1, keepdims=True)

    kept = as_column(kept_row)
    flag_lanes = jnp.concatenate([jnp.zeros((1, 64), jnp.float32), flag_row], axis=1)
    fsend[...] = jnp.concatenate([kept_row, jnp.zeros((1, 128 - ROWS), jnp.float32)], axis=1)

    def mine(chip, core, lo, n):
        return x[order_s[2 * chip + core], lo : lo + n] * kept[lo : lo + n]

    for s in loads:
        s.wait()
    pl.semaphore_wait(barrier, 78)

    d_copies = {}
    for d in D_ORDER:
        chip = lax.rem(y + d, 8)
        dsend[d] = mine(chip, other, 0, ROWS)
        cp = pltpu.make_async_remote_copy(
            src_ref=dsend.at[d], dst_ref=drecv.at[d], send_sem=d_ss.at[d], recv_sem=d_rs.at[d],
            device_id={"c": other}, device_id_type=MESH,
        )
        cp.start()
        d_copies[d] = cp
    f_copy = pltpu.make_async_remote_copy(
        src_ref=fsend, dst_ref=frecv, send_sem=f_ss, recv_sem=f_rs,
        device_id={"c": other}, device_id_type=MESH,
    )
    f_copy.start()

    def on_chip(d, half):
        chip = lax.rem(y + d, 8)
        lo = half * HALF
        return mine(chip, c, lo, HALF) + drecv[d, lo : lo + HALF]

    seen = set()
    sends = []
    waited = set()

    def ring_copy(way, k, half):
        lo = half * HALF
        i = (way * 4 + (k - 1)) * 2 + half
        to = lax.rem(y + (1 if way == 0 else 7), 8)
        return pltpu.make_async_remote_copy(
            src_ref=ring_send.at[way, k - 1, pl.ds(lo, HALF)],
            dst_ref=ring_recv.at[way, k - 1, pl.ds(lo, HALF)],
            send_sem=r_ss.at[i], recv_sem=r_rs.at[i],
            device_id={"y": to}, device_id_type=MESH,
        )

    def stage(way, k, half):
        d = k if way == 0 else 8 - k
        if d not in seen:
            d_copies[d].wait_recv()
            seen.add(d)
        lo = half * HALF
        value = on_chip(d, half)
        top = 4 if half == way else 3
        if k < top:
            ring_copy(way, k + 1, half).wait_recv()
            value = value + ring_recv[way, k, lo : lo + HALF]
        ring_send[way, k - 1, lo : lo + HALF] = value
        cp = ring_copy(way, k, half)
        cp.start()
        sends.append(cp)

    c_copies = []
    for i in range(7):
        stage(0, *UP[i])
        stage(1, *DOWN[i])
        if i == 1:
            f_copy.wait_recv()
            csend[...] = fsend[...] + frecv[...]
            for o in range(1, 8):
                cp = pltpu.make_async_remote_copy(
                    src_ref=csend, dst_ref=crecv.at[o], send_sem=c_ss.at[o], recv_sem=c_rs.at[o],
                    device_id={"y": lax.rem(y + o, 8)}, device_id_type=MESH,
                )
                cp.start()
                c_copies.append(cp)

    for cp in c_copies:
        cp.wait_recv()
    count_row = csend[...]
    for o in range(1, 8):
        count_row = count_row + crecv[o]
    count = jnp.maximum(as_column(count_row[:, :ROWS]), 1.0)

    d_copies[0].wait_recv()
    squares = jnp.zeros((8, COLS), jnp.float32)
    means = []
    for half in (1, 0):
        lo = half * HALF
        part = on_chip(0, half)
        for way in ((0, 1) if half else (1, 0)):
            ring_copy(way, 1, half).wait_recv()
            part = part + ring_recv[way, 0, lo : lo + HALF]
        mean = part / count[lo : lo + HALF]
        means.append(mean)
        sq = mean * mean
        for r in range(0, HALF, 8):
            squares = squares + sq[r : r + 8]
    mean = jnp.concatenate([means[1], means[0]], axis=0)
    squares = squares[:, 0:128] + squares[:, 128:256] + squares[:, 256:384] + squares[:, 384:512]
    squares = jnp.sum(squares, axis=0, keepdims=True)

    low = lax.broadcasted_iota(jnp.int32, (1, 128), 1) < 64
    message = jnp.where(low, squares + pltpu.roll(squares, 64, 1), flag_lanes)

    def exchange(slots, peers, message, out, into, ss, rs):
        out[...] = message
        into[0:1] = message
        for o, peer in zip(slots, peers):
            cp = pltpu.make_async_remote_copy(
                src_ref=out, dst_ref=into.at[pl.ds(o, 1)], send_sem=ss, recv_sem=rs,
                device_id=peer, device_id_type=MESH,
            )
            cp.start()
        n = len(slots)
        everything = pltpu.make_async_remote_copy(
            src_ref=into.at[pl.ds(0, n)], dst_ref=into.at[pl.ds(0, n)], send_sem=ss, recv_sem=rs,
            device_id=peers[0], device_id_type=MESH,
        )
        everything.wait_recv()
        sends.append(everything)
        return jnp.sum(into[...], axis=0, keepdims=True)

    message = exchange(range(1, 16), line, message, lsend, lrecv, n_ss.at[0], n_rs.at[0])
    message = exchange(PLANE_ORDER, plane, message, psend, precv, n_ss.at[1], n_rs.at[1])
    total = jnp.sum(jnp.where(low, message, 0.0), axis=1, keepdims=True)
    dropped = jnp.sum(jnp.where(low, 0.0, message), axis=1, keepdims=True)
    rms = jnp.sqrt(total / ENTRIES)
    clip = jnp.minimum(1.0, 0.05 / (rms + 1e-6))
    out_drop[...] = dropped[0, 0].astype(jnp.int32)

    t = steps[...]

    def power(base):
        result, factor = jnp.float32(1.0), jnp.float32(base)
        for bit in range(5):
            result = jnp.where(((t >> bit) & 1) == 1, result * factor, result)
            factor = factor * factor
        return result

    out_b1[...] = jnp.full((ROWS, COLS), 1.0 - power(0.9), jnp.float32)
    out_b2[...] = jnp.full((ROWS, COLS), 1.0 - power(0.999), jnp.float32)
    out_g[...] = mean * clip

    f_copy.wait_send()
    for cp in (*d_copies.values(), *c_copies, *sends):
        cp.wait_send()


def body(grad_parts, drop_flags, owner_order, step_count, master, moment_m, moment_v):
    block = jax.ShapeDtypeStruct((ROWS, COLS), jnp.float32)
    dma = pltpu.SemaphoreType.DMA
    vmem = pl.BlockSpec(memory_space=pltpu.VMEM)
    smem = pl.BlockSpec(memory_space=pltpu.SMEM)
    hbm = pl.BlockSpec(memory_space=pltpu.HBM)
    f32 = jnp.float32
    g, bias1, bias2, dropped = pl.pallas_call(
        kernel,
        out_shape=(block, block, block, jax.ShapeDtypeStruct((), jnp.int32)),
        in_specs=[hbm, smem, hbm, hbm],
        out_specs=(vmem, vmem, vmem, smem),
        scratch_shapes=[
            pltpu.SMEM((2 * Y,), jnp.int32),
            pltpu.VMEM((1, ROWS), jnp.int32),
            pltpu.VMEM((2 * Y, ROWS, COLS), f32),
            pltpu.VMEM((8, ROWS, COLS), f32),
            pltpu.VMEM((8, ROWS, COLS), f32),
            pltpu.VMEM((2, 4, ROWS, COLS), f32),
            pltpu.VMEM((2, 4, ROWS, COLS), f32),
            pltpu.VMEM((1, 128), f32),
            pltpu.VMEM((1, 128), f32),
            pltpu.VMEM((1, 128), f32),
            pltpu.VMEM((8, 1, 128), f32),
            pltpu.VMEM((1, 128), f32),
            pltpu.VMEM((16, 128), f32),
            pltpu.VMEM((1, 128), f32),
            pltpu.VMEM((64, 128), f32),
            dma((16,)), dma((2,)), dma((8,)), dma((8,)), dma((16,)), dma((16,)),
            dma, dma, dma((8,)), dma((8,)), dma((2,)), dma((2,)),
        ],
        compiler_params=pltpu.CompilerParams(
            collective_id=0, has_side_effects=True, vmem_limit_bytes=16 << 20
        ),
        name="clipped_adamw",
    )(
        pltpu.with_memory_space_constraint(owner_order, pltpu.HBM),
        step_count,
        pltpu.with_memory_space_constraint(drop_flags.reshape(1, ROWS), pltpu.HBM),
        pltpu.with_memory_space_constraint(grad_parts.reshape(ROWS, WIDTH), pltpu.HBM),
    )
    g = g.reshape(master.shape)
    new_m = 0.9 * moment_m + 0.1 * g
    new_v = 0.999 * moment_v + 0.001 * g * g
    m_hat = new_m / bias1.reshape(master.shape)
    v_hat = new_v / bias2.reshape(master.shape)
    direction = m_hat / (jnp.sqrt(v_hat) + 1e-8) + 0.1 * master
    new_master = master - 0.001 * direction
    return new_master, new_m, new_v, direction, dropped


def solution(mesh):
    finer = Mesh(
        mesh.devices.reshape(Y, 2, mesh.shape["tensor"], mesh.shape["pipe"]),
        ("y", "c", "tensor", "pipe"),
    )
    dp = ("y", "c")
    state = P("pipe", "tensor", None, dp)
    return jax.shard_map(
        body,
        mesh=finer,
        in_specs=(
            P(dp, "pipe", "tensor", None, None), P(dp, "pipe", "tensor", None), P(), P(),
            state, state, state,
        ),
        out_specs=(state, state, state, state, P()),
        check_vma=False,
    )
```

```python
import jax
import jax.numpy as jnp
from jax import lax
from jax.experimental import pallas as pl
from jax.experimental.pallas import tpu as pltpu
from jax.sharding import Mesh
from jax.sharding import PartitionSpec as P

MESH = pl.DeviceIdType.MESH
Y = 8
ROWS, COLS = 64, 512
WIDTH = 2 * Y * COLS
PIECES = 4
PIECE = ROWS // PIECES
ENTRIES = 33554432.0

SHORT = 1 + 7 + 15 + 63

PLANE = [8 * dx + dz for dz in (1, 2, 3, 4, 5, 6, 7, 0) for dx in (4, 3, 5, 2, 6, 1, 7, 0) if dx or dz]

D_ORDER = (4, 3, 5, 2, 6, 1, 7, 0)
SLOT = {d: i for i, d in enumerate(D_ORDER)}
GROUPS = ((0, 1), (1, 2), (3, 2), (5, 2), (7, 1))
GROUP = (0, 1, 1, 2, 2, 3, 3, 4)
FIRST, SECOND = tuple(range(PIECES // 2)), tuple(range(PIECES // 2, PIECES))


def ring_order(long, short):
    order = [(4, p) for p in long]
    for k in (3, 2, 1):
        order += [(k, p) for p in short] + [(k, p) for p in long]
    return order


WAYS = (ring_order(FIRST, SECOND), ring_order(SECOND, FIRST))
LONG = (FIRST, SECOND)


def kernel(
    order, steps, flags, grad, out_g, out_b1, out_b2, out_drop,
    order_s, flags_v, x, dsend, drecv, ring_send, ring_recv, fsend, frecv, csend, crecv, lsend, lrecv, xsend, xrecv,
    tally, load_sem, small_sem, d_ss, d_rs, r_ss, r_rs, small_ss, f_rs, c_rs, n_rs, ready,
):
    y = lax.axis_index("y")
    c = lax.axis_index("c")
    tx = lax.axis_index("tensor")
    pz = lax.axis_index("pipe")
    other = 1 - c

    smalls = [
        pltpu.make_async_copy(ref, to, small_sem.at[i])
        for i, (ref, to) in enumerate(((flags, flags_v), (order, order_s)))
    ]
    for s in smalls:
        s.start()
    loads = [
        pltpu.make_async_copy(grad.at[:, pl.ds(b * COLS, COLS)], x.at[b], load_sem)
        for b in range(2 * Y)
    ]
    for s in loads:
        s.start()
    line = [{"c": other}] + [
        {"y": lax.rem(y + o // 2, 8), "c": lax.rem(c + o % 2, 2)} for o in range(2, 16)
    ]
    along_x = [{"tensor": lax.rem(tx + o, 8)} for o in range(1, 8)]
    along_z = [{"pipe": lax.rem(pz + o, 8)} for o in range(1, 8)]
    plane = [
        {"tensor": lax.rem(tx + o // 8, 8), "pipe": lax.rem(pz + o % 8, 8)} for o in PLANE
    ]
    barrier = pltpu.get_barrier_semaphore()
    for peer in line + along_x + along_z:
        pl.semaphore_signal(barrier, inc=1, device_id=peer, device_id_type=MESH)

    for s in smalls:
        s.wait()
    flag_row = flags_v[...].astype(jnp.float32)
    kept_row = 1.0 - flag_row
    eye = lax.broadcasted_iota(jnp.int32, (ROWS, ROWS), 0) == lax.broadcasted_iota(
        jnp.int32, (ROWS, ROWS), 1
    )

    def as_column(row):
        return jnp.sum(jnp.where(eye, jnp.broadcast_to(row, (ROWS, ROWS)), 0.0), axis=1, keepdims=True)

    kept = as_column(kept_row)
    flag_lanes = jnp.concatenate([jnp.zeros((1, 64), jnp.float32), flag_row], axis=1)
    fsend[...] = jnp.concatenate([kept_row, jnp.zeros((1, 128 - ROWS), jnp.float32)], axis=1)

    def mine(chip, core, lo, n):
        return x[order_s[2 * chip + core], lo : lo + n] * kept[lo : lo + n]

    pltpu.make_async_copy(x, x, load_sem).wait()
    pl.semaphore_wait(barrier, 29)
    for peer in along_x:
        pl.semaphore_signal(ready, inc=1, device_id=peer, device_id_type=MESH)

    for slot, d in enumerate(D_ORDER):
        dsend[slot] = mine(lax.rem(y + d, 8), other, 0, ROWS)
        pltpu.make_async_remote_copy(
            src_ref=dsend.at[slot], dst_ref=drecv.at[slot], send_sem=d_ss, recv_sem=d_rs.at[GROUP[slot]],
            device_id={"c": other}, device_id_type=MESH,
        ).start()
    f_copy = pltpu.make_async_remote_copy(
        src_ref=fsend, dst_ref=frecv, send_sem=small_ss, recv_sem=f_rs,
        device_id={"c": other}, device_id_type=MESH,
    )
    f_copy.start()

    def on_chip(d, piece):
        group = GROUP[SLOT[d]]
        if group not in seen:
            seen.add(group)
            slots = drecv.at[pl.ds(*GROUPS[group])]
            pltpu.make_async_remote_copy(
                src_ref=slots, dst_ref=slots, send_sem=d_ss, recv_sem=d_rs.at[group],
                device_id={"c": other}, device_id_type=MESH,
            ).wait_recv()
        lo = piece * PIECE
        return mine(lax.rem(y + d, 8), c, lo, PIECE) + drecv[SLOT[d], lo : lo + PIECE]

    seen = set()

    def ring_copy(way, k, piece):
        rows = pl.ds(piece * PIECE, PIECE)
        i = way * len(WAYS[0]) + WAYS[way].index((k, piece))
        return pltpu.make_async_remote_copy(
            src_ref=ring_send.at[way, k - 1, rows], dst_ref=ring_recv.at[way, k - 1, rows],
            send_sem=r_ss, recv_sem=r_rs.at[i],
            device_id={"y": lax.rem(y + (1 if way == 0 else 7), 8)}, device_id_type=MESH,
        )

    def stage(way, k, piece):
        lo = piece * PIECE
        value = on_chip(k if way == 0 else 8 - k, piece)
        if k < (4 if piece in LONG[way] else 3):
            ring_copy(way, k + 1, piece).wait_recv()
            value = value + ring_recv[way, k, lo : lo + PIECE]
        ring_send[way, k - 1, lo : lo + PIECE] = value
        ring_copy(way, k, piece).start()

    for i in range(len(WAYS[0])):
        stage(0, *WAYS[0][i])
        stage(1, *WAYS[1][i])
        if i == PIECES - 1:
            f_copy.wait_recv()
            csend[...] = fsend[...] + frecv[...]
            for o in range(1, 8):
                pltpu.make_async_remote_copy(
                    src_ref=csend, dst_ref=crecv.at[o], send_sem=small_ss, recv_sem=c_rs,
                    device_id={"y": lax.rem(y + o, 8)}, device_id_type=MESH,
                ).start()

    counts = crecv.at[pl.ds(1, 7)]
    pltpu.make_async_remote_copy(
        src_ref=counts, dst_ref=counts, send_sem=small_ss, recv_sem=c_rs,
        device_id={"c": other}, device_id_type=MESH,
    ).wait_recv()
    count_row = csend[...]
    for o in range(1, 8):
        count_row = count_row + crecv[o]
    count = jnp.maximum(as_column(count_row[:, :ROWS]), 1.0)

    squares = jnp.zeros((8, COLS), jnp.float32)
    means = [None] * PIECES
    for piece in (p for pair in zip(FIRST, SECOND) for p in pair):
        lo = piece * PIECE
        part = on_chip(0, piece)
        for way in ((1, 0) if piece in FIRST else (0, 1)):
            ring_copy(way, 1, piece).wait_recv()
            part = part + ring_recv[way, 0, lo : lo + PIECE]
        mean = part / count[lo : lo + PIECE]
        means[piece] = mean
        for r in range(0, PIECE, 8):
            squares = squares + mean[r : r + 8] * mean[r : r + 8]
    mean = jnp.concatenate(means, axis=0)
    squares = squares[:, 0:128] + squares[:, 128:256] + squares[:, 256:384] + squares[:, 384:512]
    squares = jnp.sum(squares, axis=0, keepdims=True)

    low = lax.broadcasted_iota(jnp.int32, (1, 128), 1) < 64
    message = jnp.where(low, squares + pltpu.roll(squares, 64, 1), flag_lanes)

    def exchange(slots, peers, message, out, into, rs):
        out[...] = message
        into[0:1] = message
        for o, peer in zip(slots, peers):
            cp = pltpu.make_async_remote_copy(
                src_ref=out, dst_ref=into.at[pl.ds(o, 1)], send_sem=small_ss, recv_sem=rs,
                device_id=peer, device_id_type=MESH,
            )
            cp.start()
        n = len(slots)
        everything = pltpu.make_async_remote_copy(
            src_ref=into.at[pl.ds(0, n)], dst_ref=into.at[pl.ds(0, n)], send_sem=small_ss, recv_sem=rs,
            device_id=peers[0], device_id_type=MESH,
        )
        everything.wait_recv()
        return jnp.sum(into[...], axis=0, keepdims=True)

    message = exchange(range(1, 16), line, message, lsend, lrecv, n_rs.at[0])
    pl.semaphore_wait(ready, 7)
    message = exchange(PLANE, plane, message, xsend, xrecv, n_rs.at[1])
    total = jnp.sum(jnp.where(low, message, 0.0), axis=1, keepdims=True)
    dropped = jnp.sum(jnp.where(low, 0.0, message), axis=1, keepdims=True)
    rms = jnp.sqrt(total / ENTRIES)
    clip = jnp.minimum(1.0, 0.05 / (rms + 1e-6))
    out_drop[...] = jnp.broadcast_to(dropped, (1, 128)).astype(jnp.int32)

    t = steps[...]

    def power(base):
        result, factor = jnp.float32(1.0), jnp.float32(base)
        for bit in range(5):
            result = jnp.where(((t >> bit) & 1) == 1, result * factor, result)
            factor = factor * factor
        return result

    out_b1[...] = jnp.full((ROWS, COLS), 1.0 - power(0.9), jnp.float32)
    out_b2[...] = jnp.full((ROWS, COLS), 1.0 - power(0.999), jnp.float32)
    out_g[...] = mean * clip

    for ref, sem in (
        (dsend, d_ss), (ring_send.at[:, :, pl.ds(0, 56)], r_ss), (tally.at[pl.ds(0, SHORT)], small_ss)
    ):
        pltpu.make_async_remote_copy(
            src_ref=ref, dst_ref=ref, send_sem=sem, recv_sem=f_rs,
            device_id={"c": other}, device_id_type=MESH,
        ).wait_send()


def body(grad_parts, drop_flags, owner_order, step_count, master, moment_m, moment_v):
    block = jax.ShapeDtypeStruct((ROWS, COLS), jnp.float32)
    dma = pltpu.SemaphoreType.DMA
    vmem = pl.BlockSpec(memory_space=pltpu.VMEM)
    smem = pl.BlockSpec(memory_space=pltpu.SMEM)
    hbm = pl.BlockSpec(memory_space=pltpu.HBM)
    f32 = jnp.float32
    g, bias1, bias2, dropped = pl.pallas_call(
        kernel,
        out_shape=(block, block, block, jax.ShapeDtypeStruct((1, 128), jnp.int32)),
        in_specs=[hbm, smem, hbm, hbm],
        out_specs=(vmem, vmem, vmem, vmem),
        scratch_shapes=[
            pltpu.SMEM((2 * Y,), jnp.int32),
            pltpu.VMEM((1, ROWS), jnp.int32),
            pltpu.VMEM((2 * Y, ROWS, COLS), f32),
            pltpu.VMEM((8, ROWS, COLS), f32),
            pltpu.VMEM((8, ROWS, COLS), f32),
            pltpu.VMEM((2, 4, ROWS, COLS), f32),
            pltpu.VMEM((2, 4, ROWS, COLS), f32),
            pltpu.VMEM((1, 128), f32),
            pltpu.VMEM((1, 128), f32),
            pltpu.VMEM((1, 128), f32),
            pltpu.VMEM((8, 1, 128), f32),
            pltpu.VMEM((1, 128), f32),
            pltpu.VMEM((16, 128), f32),
            pltpu.VMEM((1, 128), f32),
            pltpu.VMEM((64, 128), f32),
            pltpu.VMEM((SHORT + 3, 128), f32),
            dma, dma((2,)), dma, dma((5,)), dma, dma((2 * len(WAYS[0]),)), dma, dma, dma, dma((2,)),
            pltpu.SemaphoreType.REGULAR,
        ],
        compiler_params=pltpu.CompilerParams(
            collective_id=0, has_side_effects=True, vmem_limit_bytes=16 << 20
        ),
        name="clipped_adamw",
    )(
        pltpu.with_memory_space_constraint(owner_order, pltpu.HBM),
        step_count,
        pltpu.with_memory_space_constraint(drop_flags.reshape(1, ROWS), pltpu.HBM),
        pltpu.with_memory_space_constraint(grad_parts.reshape(ROWS, WIDTH), pltpu.HBM),
    )
    g = g.reshape(master.shape)
    new_m = 0.9 * moment_m + 0.1 * g
    new_v = 0.999 * moment_v + 0.001 * g * g
    m_hat = new_m / bias1.reshape(master.shape)
    v_hat = new_v / bias2.reshape(master.shape)
    direction = m_hat / (jnp.sqrt(v_hat) + 1e-8) + 0.1 * master
    new_master = master - 0.001 * direction
    return new_master, new_m, new_v, direction, dropped[0, 0]


def solution(mesh):
    finer = Mesh(
        mesh.devices.reshape(Y, 2, mesh.shape["tensor"], mesh.shape["pipe"]),
        ("y", "c", "tensor", "pipe"),
    )
    dp = ("y", "c")
    state = P("pipe", "tensor", None, dp)
    return jax.shard_map(
        body,
        mesh=finer,
        in_specs=(
            P(dp, "pipe", "tensor", None, None), P(dp, "pipe", "tensor", None), P(), P(),
            state, state, state,
        ),
        out_specs=(state, state, state, state, P()),
        check_vma=False,
    )
```

```python
import jax
import jax.numpy as jnp
from jax import lax
from jax.experimental import pallas as pl
from jax.experimental.pallas import tpu as pltpu
from jax.sharding import Mesh
from jax.sharding import PartitionSpec as P

MESH = pl.DeviceIdType.MESH
Y = 8
ROWS, COLS = 64, 512
WIDTH = 2 * Y * COLS
PIECES = 4
PIECE = ROWS // PIECES
ENTRIES = 33554432.0

SHORT = 1 + 7 + 15 + 63

LINE = [2 * dy + dc for dy in (4, 3, 5, 2, 6, 1, 7, 0) for dc in (0, 1) if dy or dc]

PLANE = [8 * dx + dz for dz in (1, 2, 3, 4, 5, 6, 7, 0) for dx in (4, 3, 5, 2, 6, 1, 7, 0) if dx or dz]

D_ORDER = (4, 3, 5, 2, 6, 1, 7, 0)
SLOT = {d: i for i, d in enumerate(D_ORDER)}
GROUPS = ((0, 1), (1, 2), (3, 2), (5, 2), (7, 1))
GROUP = (0, 1, 1, 2, 2, 3, 3, 4)
FIRST, SECOND = tuple(range(PIECES // 2)), tuple(range(PIECES // 2, PIECES))


def ring_order(long, short):
    order = [(4, p) for p in long]
    for k in (3, 2, 1):
        order += [(k, p) for p in short] + [(k, p) for p in long]
    return order


WAYS = (ring_order(FIRST, SECOND), ring_order(SECOND, FIRST))
LONG = (FIRST, SECOND)


def kernel(
    order, steps, flags, grad, out_g, out_b1, out_b2, out_drop,
    order_s, flags_v, x, dsend, drecv, ring_send, ring_recv, fsend, frecv, csend, cpass, crecv, lsend, lrecv, xsend, xrecv,
    tally, load_sem, small_sem, d_ss, d_rs, r_ss, r_rs, small_ss, f_rs, c_rs, n_rs, ready,
):
    y = lax.axis_index("y")
    c = lax.axis_index("c")
    tx = lax.axis_index("tensor")
    pz = lax.axis_index("pipe")
    other = 1 - c

    smalls = [
        pltpu.make_async_copy(ref, to, small_sem.at[i])
        for i, (ref, to) in enumerate(((flags, flags_v), (order, order_s)))
    ]
    for s in smalls:
        s.start()
    loads = [
        pltpu.make_async_copy(grad.at[:, pl.ds(b * COLS, COLS)], x.at[b], load_sem)
        for b in range(2 * Y)
    ]
    for s in loads:
        s.start()
    line = [{"y": lax.rem(y + o // 2, 8), "c": lax.rem(c + o % 2, 2)} for o in LINE]
    along_x = [{"tensor": lax.rem(tx + o, 8)} for o in range(1, 8)]
    beside_y = [{"y": lax.rem(y + o, 8)} for o in (1, 7)]
    beside_z = [{"pipe": lax.rem(pz + o, 8)} for o in (1, 7)]
    plane = [
        {"tensor": lax.rem(tx + o // 8, 8), "pipe": lax.rem(pz + o % 8, 8)} for o in PLANE
    ]
    barrier = pltpu.get_barrier_semaphore()
    for peer in beside_y + [{"c": other}] + beside_z + along_x:
        pl.semaphore_signal(barrier, inc=1, device_id=peer, device_id_type=MESH)

    for s in smalls:
        s.wait()
    flag_row = flags_v[...].astype(jnp.float32)
    kept_row = 1.0 - flag_row
    eye = lax.broadcasted_iota(jnp.int32, (ROWS, ROWS), 0) == lax.broadcasted_iota(
        jnp.int32, (ROWS, ROWS), 1
    )

    def as_column(row):
        return jnp.sum(jnp.where(eye, jnp.broadcast_to(row, (ROWS, ROWS)), 0.0), axis=1, keepdims=True)

    kept = as_column(kept_row)
    flag_lanes = jnp.concatenate([jnp.zeros((1, 64), jnp.float32), flag_row], axis=1)
    fsend[...] = jnp.concatenate([kept_row, jnp.zeros((1, 128 - ROWS), jnp.float32)], axis=1)

    def mine(chip, core, lo, n):
        return x[order_s[2 * chip + core], lo : lo + n] * kept[lo : lo + n]

    pltpu.make_async_copy(x, x, load_sem).wait()
    pl.semaphore_wait(barrier, 12)

    def tell(peers, i):
        for peer in peers:
            pl.semaphore_signal(ready.at[i], inc=1, device_id=peer, device_id_type=MESH)

    tell(beside_z, 0)

    f_copy = pltpu.make_async_remote_copy(
        src_ref=fsend, dst_ref=frecv, send_sem=small_ss, recv_sem=f_rs,
        device_id={"c": other}, device_id_type=MESH,
    )
    f_copy.start()

    for slot, d in enumerate(D_ORDER):
        dsend[slot] = mine(lax.rem(y + d, 8), other, 0, ROWS)
        pltpu.make_async_remote_copy(
            src_ref=dsend.at[slot], dst_ref=drecv.at[slot], send_sem=d_ss, recv_sem=d_rs.at[GROUP[slot]],
            device_id={"c": other}, device_id_type=MESH,
        ).start()
    def on_chip(d, piece):
        group = GROUP[SLOT[d]]
        if group not in seen:
            seen.add(group)
            slots = drecv.at[pl.ds(*GROUPS[group])]
            pltpu.make_async_remote_copy(
                src_ref=slots, dst_ref=slots, send_sem=d_ss, recv_sem=d_rs.at[group],
                device_id={"c": other}, device_id_type=MESH,
            ).wait_recv()
        lo = piece * PIECE
        return mine(lax.rem(y + d, 8), c, lo, PIECE) + drecv[SLOT[d], lo : lo + PIECE]

    seen = set()

    def ring_copy(way, k, piece):
        rows = pl.ds(piece * PIECE, PIECE)
        i = way * len(WAYS[0]) + WAYS[way].index((k, piece))
        return pltpu.make_async_remote_copy(
            src_ref=ring_send.at[way, k - 1, rows], dst_ref=ring_recv.at[way, k - 1, rows],
            send_sem=r_ss, recv_sem=r_rs.at[i],
            device_id={"y": lax.rem(y + (1 if way == 0 else 7), 8)}, device_id_type=MESH,
        )

    def count_copy(way, k):
        return pltpu.make_async_remote_copy(
            src_ref=cpass.at[way, k - 1], dst_ref=crecv.at[way, k - 1],
            send_sem=small_ss, recv_sem=c_rs.at[way * 4 + k - 1],
            device_id={"y": lax.rem(y + (1 if way == 0 else 7), 8)}, device_id_type=MESH,
        )

    def stage(way, k, piece):
        lo = piece * PIECE
        value = on_chip(k if way == 0 else 8 - k, piece)
        if k < (4 if piece in LONG[way] else 3):
            ring_copy(way, k + 1, piece).wait_recv()
            value = value + ring_recv[way, k, lo : lo + PIECE]
        ring_send[way, k - 1, lo : lo + PIECE] = value
        ring_copy(way, k, piece).start()
        if piece == 0:
            kept_rows = csend[...]
            if k < 4 - way:
                count_copy(way, k + 1).wait_recv()
                kept_rows = kept_rows + crecv[way, k]
            cpass[way, k - 1] = kept_rows
            count_copy(way, k).start()

    t = steps[...]

    def power(base):
        result, factor = jnp.float32(1.0), jnp.float32(base)
        for bit in range(5):
            result = jnp.where(((t >> bit) & 1) == 1, result * factor, result)
            factor = factor * factor
        return result

    def bias(out, base):
        out[...] = jnp.full((ROWS, COLS), 1.0 - power(base), jnp.float32)

    f_copy.wait_recv()
    csend[...] = fsend[...] + frecv[...]
    rounds = len(WAYS[0])
    for i in range(rounds):
        stage(0, *WAYS[0][i])
        stage(1, *WAYS[1][i])
        if i == PIECES:
            bias(out_b1, 0.9)
            bias(out_b2, 0.999)
        if i >= rounds - 3:
            step = i - (rounds - 3)
            pl.semaphore_wait(ready.at[step], 2)
            tell(along_x if step == 2 else beside_z, step + 1)

    count_copy(0, 1).wait_recv()
    count_copy(1, 1).wait_recv()
    count_row = csend[...] + crecv[0, 0] + crecv[1, 0]
    count = jnp.maximum(as_column(count_row[:, :ROWS]), 1.0)

    squares = jnp.zeros((8, COLS), jnp.float32)
    means = [None] * PIECES
    for piece in (p for pair in zip(FIRST, SECOND) for p in pair):
        lo = piece * PIECE
        part = on_chip(0, piece)
        for way in ((1, 0) if piece in FIRST else (0, 1)):
            ring_copy(way, 1, piece).wait_recv()
            part = part + ring_recv[way, 0, lo : lo + PIECE]
        mean = part / count[lo : lo + PIECE]
        means[piece] = mean
        for r in range(0, PIECE, 8):
            squares = squares + mean[r : r + 8] * mean[r : r + 8]
    mean = jnp.concatenate(means, axis=0)
    squares = squares[:, 0:128] + squares[:, 128:256] + squares[:, 256:384] + squares[:, 384:512]
    squares = jnp.sum(squares, axis=0, keepdims=True)

    low = lax.broadcasted_iota(jnp.int32, (1, 128), 1) < 64
    message = jnp.where(low, squares + pltpu.roll(squares, 64, 1), flag_lanes)

    def exchange(slots, peers, message, out, into, rs):
        out[...] = message
        into[0:1] = message
        for o, peer in zip(slots, peers):
            cp = pltpu.make_async_remote_copy(
                src_ref=out, dst_ref=into.at[pl.ds(o, 1)], send_sem=small_ss, recv_sem=rs,
                device_id=peer, device_id_type=MESH,
            )
            cp.start()
        n = len(slots)
        everything = pltpu.make_async_remote_copy(
            src_ref=into.at[pl.ds(0, n)], dst_ref=into.at[pl.ds(0, n)], send_sem=small_ss, recv_sem=rs,
            device_id=peers[0], device_id_type=MESH,
        )
        everything.wait_recv()
        return jnp.sum(into[...], axis=0, keepdims=True)

    message = exchange(LINE, line, message, lsend, lrecv, n_rs.at[0])
    pl.semaphore_wait(ready.at[3], 7)
    message = exchange(PLANE, plane, message, xsend, xrecv, n_rs.at[1])
    total = jnp.sum(jnp.where(low, message, 0.0), axis=1, keepdims=True)
    dropped = jnp.sum(jnp.where(low, 0.0, message), axis=1, keepdims=True)
    rms = jnp.sqrt(total / ENTRIES)
    clip = jnp.minimum(1.0, 0.05 / (rms + 1e-6))
    out_drop[...] = jnp.broadcast_to(dropped, (1, 128)).astype(jnp.int32)

    out_g[...] = mean * clip

    for ref, sem in (
        (dsend, d_ss), (ring_send.at[:, :, pl.ds(0, 56)], r_ss), (tally.at[pl.ds(0, SHORT)], small_ss)
    ):
        pltpu.make_async_remote_copy(
            src_ref=ref, dst_ref=ref, send_sem=sem, recv_sem=f_rs,
            device_id={"c": other}, device_id_type=MESH,
        ).wait_send()


def body(grad_parts, drop_flags, owner_order, step_count, master, moment_m, moment_v):
    block = jax.ShapeDtypeStruct((ROWS, COLS), jnp.float32)
    dma = pltpu.SemaphoreType.DMA
    vmem = pl.BlockSpec(memory_space=pltpu.VMEM)
    smem = pl.BlockSpec(memory_space=pltpu.SMEM)
    hbm = pl.BlockSpec(memory_space=pltpu.HBM)
    f32 = jnp.float32
    g, bias1, bias2, dropped = pl.pallas_call(
        kernel,
        out_shape=(block, block, block, jax.ShapeDtypeStruct((1, 128), jnp.int32)),
        in_specs=[hbm, smem, hbm, hbm],
        out_specs=(vmem, vmem, vmem, vmem),
        scratch_shapes=[
            pltpu.SMEM((2 * Y,), jnp.int32),
            pltpu.VMEM((1, ROWS), jnp.int32),
            pltpu.VMEM((2 * Y, ROWS, COLS), f32),
            pltpu.VMEM((8, ROWS, COLS), f32),
            pltpu.VMEM((8, ROWS, COLS), f32),
            pltpu.VMEM((2, 4, ROWS, COLS), f32),
            pltpu.VMEM((2, 4, ROWS, COLS), f32),
            pltpu.VMEM((1, 128), f32),
            pltpu.VMEM((1, 128), f32),
            pltpu.VMEM((1, 128), f32),
            pltpu.VMEM((2, 4, 1, 128), f32),
            pltpu.VMEM((2, 4, 1, 128), f32),
            pltpu.VMEM((1, 128), f32),
            pltpu.VMEM((16, 128), f32),
            pltpu.VMEM((1, 128), f32),
            pltpu.VMEM((64, 128), f32),
            pltpu.VMEM((SHORT + 3, 128), f32),
            dma, dma((2,)), dma, dma((5,)), dma, dma((2 * len(WAYS[0]),)), dma, dma, dma((8,)), dma((2,)),
            pltpu.SemaphoreType.REGULAR((4,)),
        ],
        compiler_params=pltpu.CompilerParams(
            collective_id=0, has_side_effects=True, vmem_limit_bytes=16 << 20
        ),
        name="clipped_adamw",
    )(
        pltpu.with_memory_space_constraint(owner_order, pltpu.HBM),
        step_count,
        pltpu.with_memory_space_constraint(drop_flags.reshape(1, ROWS), pltpu.HBM),
        pltpu.with_memory_space_constraint(grad_parts.reshape(ROWS, WIDTH), pltpu.HBM),
    )
    g = g.reshape(master.shape)
    new_m = 0.9 * moment_m + 0.1 * g
    new_v = 0.999 * moment_v + 0.001 * g * g
    m_hat = new_m / bias1.reshape(master.shape)
    v_hat = new_v / bias2.reshape(master.shape)
    direction = m_hat / (jnp.sqrt(v_hat) + 1e-8) + 0.1 * master
    new_master = master - 0.001 * direction
    return new_master, new_m, new_v, direction, dropped[0, 0]


def solution(mesh):
    finer = Mesh(
        mesh.devices.reshape(Y, 2, mesh.shape["tensor"], mesh.shape["pipe"]),
        ("y", "c", "tensor", "pipe"),
    )
    dp = ("y", "c")
    state = P("pipe", "tensor", None, dp)
    return jax.shard_map(
        body,
        mesh=finer,
        in_specs=(
            P(dp, "pipe", "tensor", None, None), P(dp, "pipe", "tensor", None), P(), P(),
            state, state, state,
        ),
        out_specs=(state, state, state, state, P()),
        check_vma=False,
    )
```
